32 devices in a mesh: ens: 2 (over y), space: 4 (over z), tm: 2 (over x), mom: 2 (over core).
Axes of the slice: x: 2, y: 2, z: 4, core: 2. Of those that a mesh axis runs over, the one named last changes fastest.
Arguments:
- eigvecs: bfloat16 [8, 2, 3, 256, 2048], P(('ens', 'tm'), None, None, None, 'space'), parts along dimension 0, may hold values from -0.359375 to 0.359375
- momenta: int32 [4, 3], P('mom'), may hold values from 1 to 2
- pairs: int32 [2, 2], replicated, may hold values from 0 to 3, as said below
- spin_weights: float32 [4, 4], replicated, may hold values from -1 to 1
- perambulators: bfloat16 [4, 2, 4, 4, 256, 256], P(('ens', 'tm'), None, None, None, 'space'), parts along dimension 0, may hold values from -0.0234375 to 0.0234375
Outputs:
- blocks: bfloat16 [4, 4, 2, 256, 256], P(('ens', 'tm'), 'mom', None, 'space'), parts along dimension 0
The draws below stay inside these ranges and needn't reach their ends.
There are 2 independent parts, one for each index of `ens`. The reference program is written for one: setup_inputs(seed, part) draws one part's arguments, and reference() takes and returns one part's arrays. A program takes and returns all parts, laid end to end along the dimension named above; an argument that names none is the same for every part. Nothing has to cross between parts.
Inputs may be any that keep to these rules, and one draw needn't show every extreme that they name: pairs[q, 0], the sink, lies in time group q: (q) * 2 <= pairs[q, 0] < (q + 1) * 2; pairs[q, 1], the source, is any timeslice.
All inputs are finite; a program needn't handle non-finite values.
Results may differ from the reference program's by a relative error of at most 0.008.
Values may be sent and summed in bfloat16 or wider, within the bound.
A program may use at most 64 MiB of HBM per device.

```python
import math
import jax
import jax.numpy as jnp
from jax import lax

NV = 256
SPIN = 4
LAT = 48
T_DEV = 2
PAIR_DEV = 1
SITES = 2048
TIMES = 4
NMOM = 4
PAIRS = 2


def draw_pairs(key, part):
    base = jax.random.fold_in(key, 71)
    first_key, second_key = jax.random.split(base)
    owners = jnp.arange(PAIRS, dtype=jnp.int32) // PAIR_DEV
    sinks = owners * T_DEV + jax.random.randint(first_key, (PAIRS,), 0, T_DEV, dtype=jnp.int32)
    sources = jax.random.randint(second_key, (PAIRS,), 0, TIMES, dtype=jnp.int32)
    sources = sources.at[0].set(TIMES - 1)
    sources = sources.at[PAIRS - 1].set(0)
    return jnp.stack([sinks, sources], 1).astype(jnp.int32)


def touch_ends(drawn, key, low, top_value):
    extent = drawn.shape
    spot = [jax.random.randint(jax.random.fold_in(key, axis), (), 0, extent[axis]) for axis in range(len(extent))]
    drawn = drawn.at[tuple(spot)].set(low)
    longest = extent.index(max(extent))
    spot[longest] = (spot[longest] + 1) % extent[longest]
    return drawn.at[tuple(spot)].set(top_value)


def steps_of(rng, extent, pieces, smallest, largest):
    factor_of = 1.0
    for position, parts in pieces:
        heights = jax.random.uniform(jax.random.fold_in(jax.random.fold_in(rng, 6), position), (parts,), jnp.float32, smallest / len(pieces), largest / len(pieces))
        factor_of = factor_of * jnp.repeat(jnp.exp(heights), extent[position] // parts).reshape((-1,) + (1,) * (len(extent) - 1 - position))
    return factor_of


def scatter_about(stream_key, dims, width, bound, cuts=(), held_as=jnp.bfloat16):
    drawn = width * jax.random.normal(stream_key, dims, jnp.float32)
    if cuts:
        drawn = drawn * steps_of(stream_key, dims, cuts, -0.22, 0.18)
    return jnp.clip(drawn, -bound, bound).astype(held_as)


def setup_inputs(seed: int = 0, part: int = 0) -> dict:
    seeds = jax.random.split(jax.random.key(seed), 6)
    part_keys = jax.random.split(jax.random.fold_in(seeds[5], part), 6)
    eigvecs = scatter_about(part_keys[0], (TIMES, 2, 3, NV, SITES), 0.06, 0.359375, ((0, 2), (4, 4)))
    momenta = touch_ends(jax.random.randint(seeds[1], (NMOM, 3), 1, 3), jax.random.fold_in(seeds[1], 1), 1, 2).astype(jnp.int32)
    pairs = draw_pairs(jax.random.fold_in(seeds[5], 71), part)
    spin_weights = scatter_about(seeds[3], (SPIN, SPIN), 0.25, 1.0, (), jnp.float32)
    perambulators = scatter_about(part_keys[4], (PAIRS, 2, SPIN, SPIN, NV, NV), (NV * NV) ** -0.5, 0.0234375, ((0, 2), (4, 4)))
    return dict(eigvecs=eigvecs, momenta=momenta, pairs=pairs, spin_weights=spin_weights, perambulators=perambulators)


EXACT_PRECISION = lax.Precision.HIGHEST


def phases(momenta, site_ids):
    xcoord = (site_ids % LAT).astype(jnp.float32)
    ycoord = ((site_ids // LAT) % LAT).astype(jnp.float32)
    zcoord = (site_ids // (LAT * LAT)).astype(jnp.float32)
    mom_float = momenta.astype(jnp.float32)
    angles = (mom_float[:, 0:1] * xcoord + mom_float[:, 1:2] * ycoord + mom_float[:, 2:3] * zcoord) * (2.0 * math.pi / LAT)
    return jnp.cos(angles), jnp.sin(angles)


def contract(left_array, right_array):
    return jnp.einsum('cis,cjs->ij', left_array, right_array, precision=EXACT_PRECISION)


def elemental_table(eigvecs, cosine_rows, sine_rows):
    def one_time(vector):
        real_wide = vector[0].astype(jnp.float32)
        imag_wide = vector[1].astype(jnp.float32)

        def one_mom(phase_pair):
            cosine, sine = phase_pair
            real_turned = (cosine * real_wide + sine * imag_wide).astype(jnp.bfloat16)
            imag_turned = (cosine * imag_wide - sine * real_wide).astype(jnp.bfloat16)
            real_turned, imag_turned = lax.optimization_barrier((real_turned, imag_turned))
            real_turned = real_turned.astype(jnp.float32)
            imag_turned = imag_turned.astype(jnp.float32)
            real_part = contract(real_wide, real_turned) + contract(imag_wide, imag_turned)
            imag_part = contract(real_wide, imag_turned) - contract(imag_wide, real_turned)
            return jnp.stack([real_part, imag_part]).astype(jnp.bfloat16)

        return lax.map(one_mom, (cosine_rows, sine_rows))

    return lax.map(one_time, eigvecs)


def bridge(mixed_block, source):
    real_part = jnp.einsum('kl,mjl->mkj', mixed_block[0], source[:, 0], precision=EXACT_PRECISION) + jnp.einsum('kl,mjl->mkj', mixed_block[1], source[:, 1], precision=EXACT_PRECISION)
    imag_part = jnp.einsum('kl,mjl->mkj', mixed_block[1], source[:, 0], precision=EXACT_PRECISION) - jnp.einsum('kl,mjl->mkj', mixed_block[0], source[:, 1], precision=EXACT_PRECISION)
    return jnp.stack([real_part, imag_part], 1).astype(jnp.bfloat16)


def attach(sink_elem, bridged):
    real_part = jnp.einsum('mik,mkj->mij', sink_elem[:, 0], bridged[:, 0], precision=EXACT_PRECISION) - jnp.einsum('mik,mkj->mij', sink_elem[:, 1], bridged[:, 1], precision=EXACT_PRECISION)
    imag_part = jnp.einsum('mik,mkj->mij', sink_elem[:, 0], bridged[:, 1], precision=EXACT_PRECISION) + jnp.einsum('mik,mkj->mij', sink_elem[:, 1], bridged[:, 0], precision=EXACT_PRECISION)
    return jnp.stack([real_part, imag_part], 1).astype(jnp.bfloat16)


def reference(eigvecs, momenta, pairs, spin_weights, perambulators):
    site_ids = jnp.arange(SITES, dtype=jnp.int32)
    cosine_rows, sine_rows = phases(momenta, site_ids)
    elementals = elemental_table(eigvecs, cosine_rows, sine_rows)
    mixed_peramb = jnp.einsum('ab,qcabkl->qckl', spin_weights.astype(jnp.float32), perambulators.astype(jnp.float32), precision=EXACT_PRECISION).astype(jnp.bfloat16)

    def one_pair(pair_item):
        pair_ids, mixed_block = pair_item
        sink_elem = elementals[pair_ids[0]].astype(jnp.float32)
        source = elementals[pair_ids[1]].astype(jnp.float32)
        bridged = bridge(mixed_block.astype(jnp.float32), source).astype(jnp.float32)
        return attach(sink_elem, bridged)

    return lax.map(one_pair, (pairs, mixed_peramb))
```

```python
import functools
import math

import jax
import jax.numpy as jnp
from jax import lax
from jax.experimental import pallas as pl
from jax.experimental.pallas import tpu as pltpu
from jax.sharding import PartitionSpec as P

LAT = 48
MESH = pl.DeviceIdType.MESH
F32 = jnp.float32
BF16 = jnp.bfloat16
NT = (((1,), (1,)), ((), ()))
ROW_BLOCK = 32


def nt_dot(left, right):
    return lax.dot_general(left, right, NT, preferred_element_type=F32)


def nn_dot(left, right):
    return jnp.dot(left, right, preferred_element_type=F32)


def flat_rows(chunks):
    count, rows, cols = chunks.shape
    if rows % 16:
        return chunks.astype(F32).reshape(count * rows, cols).astype(chunks.dtype)
    return chunks.reshape(count * rows, cols)


def pick(index, values):
    chosen = values[0]
    for which in range(1, len(values)):
        chosen = jnp.where(index == which, values[which], chosen)
    return chosen


def kernel(
    dims, pairs_ref, spin_ref, mom_ref, eig_ref, per_ref, out_ref,
    vecs, turned, trig, per_buf, part, right_out, right_in, left_out, left_in,
    reduced, swap_out, swap_in, source, mixed,
    eig_sem, per_sem, rs_send, rs_recv, swap_send, swap_recv, ag_send, ag_recv,
    mix_send, mix_recv, core_send, core_recv,
):
    (space, groups, times, moms, colours, vec_count, sites, pair_dev, spin) = dims
    rows = vec_count // space
    half = space // 2
    width = colours * sites
    me = lax.axis_index("space")
    group = lax.axis_index("tm")
    core = lax.axis_index("mom")
    right = lax.rem(me + 1, space)
    left = lax.rem(me + space - 1, space)
    other_core = 1 - core
    sent = []

    barrier = pltpu.get_barrier_semaphore()
    friends = [{"space": lax.rem(me + step, space)} for step in range(1, space)]
    friends += [{"tm": lax.rem(group + step, groups)} for step in range(1, groups)]
    friends += [{"mom": other_core}]
    for friend in friends:
        pl.semaphore_signal(barrier, inc=1, device_id=friend, device_id_type=MESH)

    def remote(src, dst, send_sem, recv_sem, target):
        return pltpu.make_async_remote_copy(
            src_ref=src, dst_ref=dst, send_sem=send_sem, recv_sem=recv_sem,
            device_id=target, device_id_type=MESH,
        )

    def launch(copy):
        copy.start()
        sent.append(copy)

    per_copy = pltpu.make_async_copy(per_ref.at[:, core], per_buf, per_sem)
    per_copy.start()
    eig_copies = []
    for t in range(times):
        of_time = []
        for c in range(2):
            for colour in range(colours):
                first = (c * colours + colour) * sites
                copy = pltpu.make_async_copy(
                    eig_ref.at[t, c, colour], vecs.at[t, :, pl.ds(first, sites)],
                    eig_sem.at[t, c, colour],
                )
                copy.start()
                of_time.append(copy)
        eig_copies.append(of_time)

    site = (lax.broadcasted_iota(jnp.int32, (8, sites), 1) + me * sites).astype(F32)
    line = jnp.floor((site + 0.5) * (1.0 / LAT))
    xcoord = site - line * LAT
    zcoord = jnp.floor((line + 0.5) * (1.0 / LAT))
    ycoord = line - zcoord * LAT
    for m in range(moms):
        turns = (
            mom_ref[m, 0].astype(F32) * xcoord
            + mom_ref[m, 1].astype(F32) * ycoord
            + mom_ref[m, 2].astype(F32) * zcoord
        )
        angle = turns * (2.0 * math.pi / LAT)
        trig[m, 0] = jnp.cos(angle)
        trig[m, 1] = jnp.sin(angle)

    per_copy.wait()
    for q in range(pair_dev):
        total = jnp.zeros((rows, vec_count), F32)
        for a in range(spin):
            for b in range(spin):
                total = total + spin_ref[a, b] * per_buf[q, a, b].astype(F32)
        mixed[me, core, q] = total.astype(BF16)

    pl.semaphore_wait(barrier, len(friends))

    def mix_hop(step, owner):
        return remote(
            mixed.at[owner, core], mixed.at[owner, core], mix_send.at[step - 1],
            mix_recv.at[step - 1], {"space": lax.rem(me + step, space)},
        )

    def core_hop(step):
        owner = lax.rem(me + space - step, space)
        return remote(
            mixed.at[owner, core], mixed.at[owner, core], core_send.at[step],
            core_recv.at[step], {"mom": other_core},
        )

    for step in range(1, space):
        launch(mix_hop(step, me))
    launch(core_hop(0))

    def build(unit, m, t):
        if m == 0:
            for copy in eig_copies[t]:
                copy.wait()
        cosine = trig[m, 0][None]
        sine = trig[m, 1][None]

        def block(step, carry):
            first = pl.multiple_of(step * ROW_BLOCK, ROW_BLOCK)
            span = pl.ds(first, ROW_BLOCK)
            for colour in range(colours):
                real_at = pl.ds(colour * sites, sites)
                imag_at = pl.ds((colours + colour) * sites, sites)
                shape = (ROW_BLOCK // 8, 8, sites)
                real = vecs[t, span, real_at].astype(F32).reshape(shape)
                imag = vecs[t, span, imag_at].astype(F32).reshape(shape)
                turned[span, real_at] = (
                    (cosine * real + sine * imag).reshape(ROW_BLOCK, sites).astype(BF16)
                )
                turned[span, imag_at] = (
                    (cosine * imag - sine * real).reshape(ROW_BLOCK, sites).astype(BF16)
                )
            return carry

        lax.fori_loop(0, vec_count // ROW_BLOCK, block, 0)
        real_part = nt_dot(vecs[t], turned[...])
        imag_part = nt_dot(vecs[t, :, :width], turned[:, width:]) - nt_dot(
            vecs[t, :, width:], turned[:, :width]
        )
        part[unit, 0] = real_part.reshape(space, rows, vec_count)
        part[unit, 1] = imag_part.reshape(space, rows, vec_count)

    def ring_copy(unit, step, way):
        out, into, target = (
            (right_out, right_in, right) if way == 0 else (left_out, left_in, left)
        )
        held = pl.ds(way, 1) if step == 1 else pl.ds(0, 2)
        return remote(
            out.at[unit, step - 1, held], into.at[unit, step - 1, held],
            rs_send.at[way, unit, step - 1], rs_recv.at[way, unit, step - 1],
            {"space": target},
        )

    def reduce_step(unit, step):
        for way in range(2):
            into, out = (right_in, right_out) if way == 0 else (left_in, left_out)
            ahead = half - step + 1
            chunk = lax.rem(me + ahead if way == 0 else me + space - ahead, space)
            if step > 1:
                ring_copy(unit, step - 1, way).wait_recv()
            for c in (way,) if step == 1 else (0, 1):
                value = part[unit, c, chunk]
                if step > 2 or (step == 2 and c == way):
                    value = value + into[unit, step - 2, c].astype(F32)
                out[unit, step - 1, c] = value.astype(BF16)
            launch(ring_copy(unit, step, way))

    def reduce_end(unit, m, t):
        for way in range(2):
            if half:
                ring_copy(unit, half, way).wait_recv()
        for c in range(2):
            value = part[unit, c, me]
            if half > 1 or (half and c == 0):
                value = value + right_in[unit, half - 1, c].astype(F32)
            if half > 1 or (half and c == 1):
                value = value + left_in[unit, half - 1, c].astype(F32)
            reduced[m, t, c] = value.astype(BF16)

    def local_time(pair, end):
        return jnp.clip(pairs_ref[pair, end] - group * times, 0, times - 1)

    def chosen_time(m, which):
        return pick(which, [reduced[m, t] for t in range(times)])

    def swap_copy(m, step):
        return remote(
            swap_out.at[m, step], swap_in.at[m, step], swap_send.at[m, step],
            swap_recv.at[m, step], {"tm": lax.rem(group + step, groups)},
        )

    def swap_start(m):
        for step in range(groups):
            owner = lax.rem(group + step, groups)
            for q in range(pair_dev):
                rows_of = chosen_time(m, local_time(owner * pair_dev + q, 1))
                swap_out[m, step, :, q] = rows_of
            if step:
                launch(swap_copy(m, step))

    def gather_copy(m, step, way):
        target = right if way == 0 else left
        chunk = lax.rem(me + space - step + 1 if way == 0 else me + step - 1, space)
        held = pl.ds(way, 1) if step == half else pl.ds(0, 2)
        return remote(
            source.at[m, chunk, held], source.at[m, chunk, held],
            ag_send.at[way, m, step - 1], ag_recv.at[way, m, step - 1],
            {"space": target},
        )

    def gather_start(m):
        for step in range(1, groups):
            swap_copy(m, step).wait_recv()
        for q in range(pair_dev):
            holder = lax.div(pairs_ref[group * pair_dev + q, 1], times)
            back = lax.rem(group + groups - holder, groups)
            held = [swap_out[m, 0, :, q]] + [swap_in[m, s, :, q] for s in range(1, groups)]
            source[m, me, :, q] = pick(back, held)
        for way in range(2):
            if half:
                launch(gather_copy(m, 1, way))

    def gather_step(m, step):
        for way in range(2):
            gather_copy(m, step - 1, way).wait_recv()
            launch(gather_copy(m, step, way))

    def sink_times_mixed(m):
        made = []
        for q in range(pair_dev):
            sink = chosen_time(m, local_time(group * pair_dev + q, 0))
            mixed_re = flat_rows(mixed[:, 0, q])
            mixed_im = flat_rows(mixed[:, 1, q])
            real_part = nn_dot(sink[0], mixed_re) - nn_dot(sink[1], mixed_im)
            imag_part = nn_dot(sink[0], mixed_im) + nn_dot(sink[1], mixed_re)
            made.append((real_part.astype(BF16), imag_part.astype(BF16)))
        return made

    def finish(m, made):
        for way in range(2):
            if half:
                gather_copy(m, half, way).wait_recv()
        for q in range(pair_dev):
            real, imag = made[q]
            source_re = flat_rows(source[m, :, 0, q])
            source_im = flat_rows(source[m, :, 1, q])
            out_ref[q, m, 0] = (nt_dot(real, source_re) + nt_dot(imag, source_im)).astype(BF16)
            out_ref[q, m, 1] = (nt_dot(imag, source_re) - nt_dot(real, source_im)).astype(BF16)

    units = [(m, t) for m in range(moms) for t in range(times)]
    lag = 2
    for unit, (m, t) in enumerate(units):
        build(unit, m, t)
        if half:
            reduce_step(unit, 1)
        if half > 1 and unit >= lag:
            reduce_step(unit - lag, 2)
    for unit in range(max(len(units) - lag, 0), len(units)):
        if half > 1:
            reduce_step(unit, 2)
    for step in range(3, half + 1):
        for unit in range(len(units)):
            reduce_step(unit, step)

    for step in range(1, space):
        mix_hop(step, me).wait_recv()
        launch(core_hop(step))

    made = []
    for unit, (m, t) in enumerate(units):
        reduce_end(unit, m, t)
        if t == times - 1:
            swap_start(m)
            if m == 0:
                for step in range(space):
                    core_hop(step).wait_recv()
            made.append(sink_times_mixed(m))
            if m:
                gather_start(m - 1)
    gather_start(moms - 1)
    for step in range(2, half + 1):
        for m in range(moms):
            gather_step(m, step)
    for m in range(moms):
        finish(m, made[m])
    for copy in sent:
        copy.wait_send()


def local(eigvecs, momenta, pairs, spin_weights, perambulators):
    times, _, colours, vec_count, sites = eigvecs.shape
    pair_dev, _, spin, _, rows, _ = perambulators.shape
    moms = momenta.shape[0]
    space = lax.axis_size("space")
    groups = lax.axis_size("tm")
    half = max(space // 2, 1)
    units = moms * times
    dims = (space, groups, times, moms, colours, vec_count, sites, pair_dev, spin)
    smem = pl.BlockSpec(memory_space=pltpu.SMEM)
    hbm = pl.BlockSpec(memory_space=pl.ANY)
    dma = pltpu.SemaphoreType.DMA
    ring = pltpu.VMEM((units, half, 2, rows, vec_count), BF16)
    swap = pltpu.VMEM((moms, groups, 2, pair_dev, rows, vec_count), BF16)
    return pl.pallas_call(
        functools.partial(kernel, dims),
        out_shape=jax.ShapeDtypeStruct((pair_dev, moms, 2, rows, vec_count), BF16),
        in_specs=[smem, smem, smem, hbm, hbm],
        out_specs=pl.BlockSpec(memory_space=pltpu.VMEM),
        scratch_shapes=[
            pltpu.VMEM((times, vec_count, 2 * colours * sites), BF16),
            pltpu.VMEM((vec_count, 2 * colours * sites), BF16),
            pltpu.VMEM((moms, 2, 8, sites), F32),
            pltpu.VMEM((pair_dev, spin, spin, rows, vec_count), BF16),
            pltpu.VMEM((units, 2, space, rows, vec_count), F32),
            ring, ring, ring, ring,
            pltpu.VMEM((moms, times, 2, rows, vec_count), BF16),
            swap, swap,
            pltpu.VMEM((moms, space, 2, pair_dev, rows, vec_count), BF16),
            pltpu.VMEM((space, 2, pair_dev, rows, vec_count), BF16),
            dma((times, 2, colours)), dma(()),
            dma((2, units, half)), dma((2, units, half)),
            dma((moms, groups)), dma((moms, groups)),
            dma((2, moms, half)), dma((2, moms, half)),
            dma((space,)), dma((space,)), dma((space,)), dma((space,)),
        ],
        compiler_params=pltpu.CompilerParams(collective_id=0, has_side_effects=True),
    )(pairs, spin_weights, momenta, eigvecs, perambulators)


def solution(mesh):
    return jax.shard_map(
        local,
        mesh=mesh,
        in_specs=(
            P(("ens", "tm"), None, None, None, "space"),
            P("mom", None),
            P(),
            P(),
            P(("ens", "tm"), None, None, None, "space", None),
        ),
        out_specs=P(("ens", "tm"), "mom", None, "space", None),
        check_vma=False,
    )
```

```python
import functools
import math

import jax
import jax.numpy as jnp
from jax import lax
from jax.experimental import pallas as pl
from jax.experimental.pallas import tpu as pltpu
from jax.sharding import PartitionSpec as P

LAT = 48
MESH = pl.DeviceIdType.MESH
F32 = jnp.float32
BF16 = jnp.bfloat16
NT = (((1,), (1,)), ((), ()))
ROW_BLOCK = 32


def nt_dot(left, right):
    return lax.dot_general(left, right, NT, preferred_element_type=F32)


def nn_dot(left, right):
    return jnp.dot(left, right, preferred_element_type=F32)


def flat_rows(chunks):
    count, rows, cols = chunks.shape
    if rows % 16:
        return chunks.astype(F32).reshape(count * rows, cols).astype(chunks.dtype)
    return chunks.reshape(count * rows, cols)


def pick(index, values):
    chosen = values[0]
    for which in range(1, len(values)):
        chosen = jnp.where(index == which, values[which], chosen)
    return chosen


def halves(value):
    high = value.astype(BF16)
    return high, (value - high.astype(F32)).astype(BF16)


def kernel(
    dims, pairs_ref, spin_ref, mom_ref, eig_ref, per_ref, out_ref,
    vecs, turned, trig, per_buf, part, right_out, right_in, left_out, left_in,
    total_buf, reduced, swap_out, swap_in, source, mixed,
    eig_sem, per_sem, rs_send, rs_recv, swap_send, swap_recv, ag_send, ag_recv,
    mix_send, mix_recv, core_send, core_recv,
):
    (space, groups, times, moms, colours, vec_count, sites, pair_dev, spin) = dims
    rows = vec_count // space
    last = space - 1
    width = colours * sites
    me = lax.axis_index("space")
    group = lax.axis_index("tm")
    core = lax.axis_index("mom")
    right = lax.rem(me + 1, space)
    left = lax.rem(me + space - 1, space)
    other_core = 1 - core
    sent = []

    barrier = pltpu.get_barrier_semaphore()
    friends = [{"space": lax.rem(me + step, space)} for step in range(1, space)]
    friends += [{"tm": lax.rem(group + step, groups)} for step in range(1, groups)]
    friends += [{"mom": other_core}]
    for friend in friends:
        pl.semaphore_signal(barrier, inc=1, device_id=friend, device_id_type=MESH)

    def remote(src, dst, send_sem, recv_sem, target):
        return pltpu.make_async_remote_copy(
            src_ref=src, dst_ref=dst, send_sem=send_sem, recv_sem=recv_sem,
            device_id=target, device_id_type=MESH,
        )

    def launch(copy):
        copy.start()
        sent.append(copy)

    per_copy = pltpu.make_async_copy(per_ref.at[:, core], per_buf, per_sem)
    per_copy.start()
    eig_copies = []
    for t in range(times):
        of_time = []
        for c in range(2):
            for colour in range(colours):
                first = (c * colours + colour) * sites
                copy = pltpu.make_async_copy(
                    eig_ref.at[t, c, colour], vecs.at[t, :, pl.ds(first, sites)],
                    eig_sem.at[t, c, colour],
                )
                copy.start()
                of_time.append(copy)
        eig_copies.append(of_time)

    site = (lax.broadcasted_iota(jnp.int32, (8, sites), 1) + me * sites).astype(F32)
    line = jnp.floor((site + 0.5) * (1.0 / LAT))
    xcoord = site - line * LAT
    zcoord = jnp.floor((line + 0.5) * (1.0 / LAT))
    ycoord = line - zcoord * LAT
    for m in range(moms):
        turns = (
            mom_ref[m, 0].astype(F32) * xcoord
            + mom_ref[m, 1].astype(F32) * ycoord
            + mom_ref[m, 2].astype(F32) * zcoord
        )
        angle = turns * (2.0 * math.pi / LAT)
        trig[m, 0] = jnp.cos(angle)
        trig[m, 1] = jnp.sin(angle)

    per_copy.wait()
    for q in range(pair_dev):
        total = jnp.zeros((rows, vec_count), F32)
        for a in range(spin):
            for b in range(spin):
                total = total + spin_ref[a, b] * per_buf[q, a, b].astype(F32)
        mixed[me, core, q] = total.astype(BF16)

    pl.semaphore_wait(barrier, len(friends))

    def mix_hop(step, owner):
        return remote(
            mixed.at[owner, core], mixed.at[owner, core], mix_send.at[step - 1],
            mix_recv.at[step - 1], {"space": lax.rem(me + step, space)},
        )

    def core_hop(step):
        owner = lax.rem(me + space - step, space)
        return remote(
            mixed.at[owner, core], mixed.at[owner, core], core_send.at[step],
            core_recv.at[step], {"mom": other_core},
        )

    for step in range(1, space):
        launch(mix_hop(step, me))
    launch(core_hop(0))

    first_time = jnp.clip(pairs_ref[group * pair_dev, 0] - group * times, 0, times - 1)

    def slot_of(pair, end):
        t = jnp.clip(pairs_ref[pair, end] - group * times, 0, times - 1)
        return lax.rem(t - first_time + times, times)

    def build(unit, m, slot):
        if unit == 0:
            for of_time in eig_copies:
                for copy in of_time:
                    copy.wait()
        t = lax.rem(first_time + slot, times)
        cosine = trig[m, 0][None]
        sine = trig[m, 1][None]

        def block(step, carry):
            first = pl.multiple_of(step * ROW_BLOCK, ROW_BLOCK)
            span = pl.ds(first, ROW_BLOCK)
            for colour in range(colours):
                real_at = pl.ds(colour * sites, sites)
                imag_at = pl.ds((colours + colour) * sites, sites)
                shape = (ROW_BLOCK // 8, 8, sites)
                real = vecs[t, span, real_at].astype(F32).reshape(shape)
                imag = vecs[t, span, imag_at].astype(F32).reshape(shape)
                turned[span, real_at] = (
                    (cosine * real + sine * imag).reshape(ROW_BLOCK, sites).astype(BF16)
                )
                turned[span, imag_at] = (
                    (cosine * imag - sine * real).reshape(ROW_BLOCK, sites).astype(BF16)
                )
            return carry

        lax.fori_loop(0, vec_count // ROW_BLOCK, block, 0)
        real_part = nt_dot(vecs[t], turned[...])
        imag_part = nt_dot(vecs[t, :, :width], turned[:, width:]) - nt_dot(
            vecs[t, :, width:], turned[:, :width]
        )
        part[unit, 0] = real_part.reshape(space, rows, vec_count)
        part[unit, 1] = imag_part.reshape(space, rows, vec_count)

    ends_first = sorted(range(space), key=lambda chunk: min(chunk, last - chunk))

    def swap_copy(m, step, chunk):
        return remote(
            swap_out.at[m, step, chunk], swap_in.at[m, step, chunk],
            swap_send.at[m, step, chunk], swap_recv.at[m, step, chunk],
            {"tm": lax.rem(group + step, groups)},
        )

    def swap_start(m):
        for chunk in ends_first:
            for step in range(1, groups):
                owner = lax.rem(group + step, groups)
                for q in range(pair_dev):
                    slot = slot_of(owner * pair_dev + q, 1)
                    for c in range(2):
                        held = [part[m * times + k, c, chunk] for k in range(times)]
                        swap_out[m, step, chunk, q, c] = pick(slot, held).astype(BF16)
                launch(swap_copy(m, step, chunk))

    def term(job, q, c, chunk):
        kind, m = jobs[job]
        pair = group * pair_dev + q
        if kind == "sink":
            if q == 0:
                return part[m * times, c, chunk]
            return pick(slot_of(pair, 0), [part[m * times + k, c, chunk] for k in range(times)])
        own = pick(slot_of(pair, 1), [part[m * times + k, c, chunk] for k in range(times)])
        holder = lax.div(pairs_ref[pair, 1], times)
        back = lax.rem(group + groups - holder, groups)
        held = [own] + [swap_in[m, step, chunk, q, c].astype(F32) for step in range(1, groups)]
        return pick(back, held)

    def await_swap(job, chunk):
        kind, m = jobs[job]
        if kind == "source":
            for step in range(1, groups):
                swap_copy(m, step, chunk).wait_recv()

    def line_copy(job, chunk, way):
        out, into, target = (
            (right_out, right_in, right) if way == 0 else (left_out, left_in, left)
        )
        return remote(
            out.at[job, chunk], into.at[job, chunk], rs_send.at[way, job, chunk],
            rs_recv.at[way, job, chunk], {"space": target},
        )

    def hop(job, chunk, way, at_end):
        out, into = (right_out, right_in) if way == 0 else (left_out, left_in)
        active = me < chunk if way == 0 else me > chunk
        end = me == 0 if way == 0 else me == last

        @pl.when(active & (end if at_end else jnp.logical_not(end)))
        def _():
            await_swap(job, chunk)
            if not at_end:
                line_copy(job, chunk, way).wait_recv()
            for q in range(pair_dev):
                for c in range(2):
                    value = term(job, q, c, chunk)
                    if not at_end:
                        value = value + into[job, chunk, q, c].astype(F32)
                    out[job, chunk, q, c] = value.astype(BF16)
            line_copy(job, chunk, way).start()

    def hops(job, at_end):
        def step(k, carry):
            hop(job, last - k, 0, at_end)
            hop(job, k, 1, at_end)
            return carry

        lax.fori_loop(0, last, step, 0)

    def reduce_end(job):
        await_swap(job, me)
        for q in range(pair_dev):
            for c in range(2):
                total_buf[q, c] = term(job, q, c, me)
        for way in range(2):
            into = right_in if way == 0 else left_in

            @pl.when(me > 0 if way == 0 else me < last)
            def _():
                line_copy(job, me, way).wait_recv()
                total_buf[...] = total_buf[...] + into[job, me].astype(F32)

        kind, m = jobs[job]
        if kind == "sink":
            reduced[m] = total_buf[...].astype(BF16)
        else:
            for c in range(2):
                source[m, me, c] = total_buf[:, c].astype(BF16)

    def gather_copy(m, chunk, way):
        return remote(
            source.at[m, chunk], source.at[m, chunk], ag_send.at[way, m, chunk],
            ag_recv.at[way, m, chunk], {"space": right if way == 0 else left},
        )

    def gather_start(m):
        @pl.when(me < last)
        def _():
            gather_copy(m, me, 0).start()

        @pl.when(me > 0)
        def _():
            gather_copy(m, me, 1).start()

    def gather_pass(m):
        def step(k, carry):
            for way in range(2):
                chunk = me - k if way == 0 else me + k

                @pl.when(chunk >= 0 if way == 0 else chunk <= last)
                def _():
                    gather_copy(m, chunk, way).wait_recv()

                    @pl.when(me < last if way == 0 else me > 0)
                    def _():
                        gather_copy(m, chunk, way).start()

            return carry

        lax.fori_loop(1, space, step, 0)

    def await_sent():
        def step(chunk, carry):
            for way in range(2):
                @pl.when(me < chunk if way == 0 else me > chunk)
                def _():
                    for job in range(len(jobs)):
                        line_copy(job, chunk, way).wait_send()

                held = (chunk <= me) & (me < last) if way == 0 else (chunk >= me) & (me > 0)

                @pl.when(held)
                def _():
                    for m in range(moms):
                        gather_copy(m, chunk, way).wait_send()

            return carry

        lax.fori_loop(0, space, step, 0)
        for copy in sent:
            copy.wait_send()

    def sink_times_mixed(m):
        made = []
        for q in range(pair_dev):
            sink = reduced[m, q]
            mixed_re = flat_rows(mixed[:, 0, q])
            mixed_im = flat_rows(mixed[:, 1, q])
            real_part = nn_dot(sink[0], mixed_re) - nn_dot(sink[1], mixed_im)
            imag_part = nn_dot(sink[0], mixed_im) + nn_dot(sink[1], mixed_re)
            made.append((halves(real_part), halves(imag_part)))
        return made

    def finish(m, made):
        for q in range(pair_dev):
            real, imag = made[q]
            source_re = flat_rows(source[m, :, 0, q])
            source_im = flat_rows(source[m, :, 1, q])

            def times_source(left, right):
                both = nt_dot(jnp.concatenate(left, 0), right)
                return both[:rows] + both[rows:]

            out_ref[q, m, 0] = (
                times_source(real, source_re) + times_source(imag, source_im)
            ).astype(BF16)
            out_ref[q, m, 1] = (
                times_source(imag, source_re) - times_source(real, source_im)
            ).astype(BF16)

    jobs = [("sink", 0)] + [("source", m) for m in range(moms)]
    jobs += [("sink", m) for m in range(1, moms)]
    sink_job = {m: jobs.index(("sink", m)) for m in range(moms)}
    source_job = {m: jobs.index(("source", m)) for m in range(moms)}
    for m in range(moms):
        for slot in range(times):
            build(m * times + slot, m, slot)
            if m == 0 and slot == 0:
                hops(sink_job[0], True)
        swap_start(m)
    hops(source_job[0], True)
    hops(sink_job[0], False)
    for step in range(1, space):
        mix_hop(step, me).wait_recv()
        launch(core_hop(step))
    for m in range(moms):
        if m + 1 < moms:
            hops(source_job[m + 1], True)
        hops(source_job[m], False)
        reduce_end(source_job[m])
        gather_start(m)
        if m + 1 < moms:
            hops(sink_job[m + 1], True)
        if m:
            gather_pass(m - 1)
    for m in range(1, moms):
        hops(sink_job[m], False)
    for step in range(space):
        core_hop(step).wait_recv()
    reduce_end(sink_job[0])
    made = [sink_times_mixed(0)]
    gather_pass(moms - 1)
    finish(0, made[0])
    for m in range(1, moms):
        reduce_end(sink_job[m])
        finish(m, sink_times_mixed(m))
    await_sent()


def local(eigvecs, momenta, pairs, spin_weights, perambulators):
    times, _, colours, vec_count, sites = eigvecs.shape
    pair_dev, _, spin, _, rows, _ = perambulators.shape
    moms = momenta.shape[0]
    space = lax.axis_size("space")
    groups = lax.axis_size("tm")
    jobs = 2 * moms
    dims = (space, groups, times, moms, colours, vec_count, sites, pair_dev, spin)
    smem = pl.BlockSpec(memory_space=pltpu.SMEM)
    hbm = pl.BlockSpec(memory_space=pl.ANY)
    dma = pltpu.SemaphoreType.DMA
    line = pltpu.VMEM((jobs, space, pair_dev, 2, rows, vec_count), BF16)
    swap = pltpu.VMEM((moms, groups, space, pair_dev, 2, rows, vec_count), BF16)
    return pl.pallas_call(
        functools.partial(kernel, dims),
        out_shape=jax.ShapeDtypeStruct((pair_dev, moms, 2, rows, vec_count), BF16),
        in_specs=[smem, smem, smem, hbm, hbm],
        out_specs=pl.BlockSpec(memory_space=pltpu.VMEM),
        scratch_shapes=[
            pltpu.VMEM((times, vec_count, 2 * colours * sites), BF16),
            pltpu.VMEM((vec_count, 2 * colours * sites), BF16),
            pltpu.VMEM((moms, 2, 8, sites), F32),
            pltpu.VMEM((pair_dev, spin, spin, rows, vec_count), BF16),
            pltpu.VMEM((moms * times, 2, space, rows, vec_count), F32),
            line, line, line, line,
            pltpu.VMEM((pair_dev, 2, rows, vec_count), F32),
            pltpu.VMEM((moms, pair_dev, 2, rows, vec_count), BF16),
            swap, swap,
            pltpu.VMEM((moms, space, 2, pair_dev, rows, vec_count), BF16),
            pltpu.VMEM((space, 2, pair_dev, rows, vec_count), BF16),
            dma((times, 2, colours)), dma(()),
            dma((2, jobs, space)), dma((2, jobs, space)),
            dma((moms, groups, space)), dma((moms, groups, space)),
            dma((2, moms, space)), dma((2, moms, space)),
            dma((space,)), dma((space,)), dma((space,)), dma((space,)),
        ],
        compiler_params=pltpu.CompilerParams(collective_id=0, has_side_effects=True),
    )(pairs, spin_weights, momenta, eigvecs, perambulators)


def solution(mesh):
    return jax.shard_map(
        local,
        mesh=mesh,
        in_specs=(
            P(("ens", "tm"), None, None, None, "space"),
            P("mom", None),
            P(),
            P(),
            P(("ens", "tm"), None, None, None, "space", None),
        ),
        out_specs=P(("ens", "tm"), "mom", None, "space", None),
        check_vma=False,
    )
```
